32 devices in a mesh: dp: 32 (over z, y, x, core).
Axes of the slice: x: 2, y: 2, z: 4, core: 2. Of those that a mesh axis runs over, the one named last changes fastest.
Arguments:
- x_in: bfloat16 [512, 192, 2048], P('dp')
- grad_y: bfloat16 [512, 192, 2048], P('dp')
- g_in: bfloat16 [2048], replicated
- w_q: bfloat16 [2048, 16, 192], replicated
- w_dkv: bfloat16 [2048, 512], replicated
- g_kv: bfloat16 [512], replicated
- w_kr: bfloat16 [2048, 64], replicated
- w_uk: bfloat16 [512, 16, 128], replicated
- w_uv: bfloat16 [512, 16, 128], replicated
- w_o: bfloat16 [16, 128, 2048], replicated
Outputs:
- output 1: bfloat16 [512, 192, 2048], P('dp')
- output 2: float32 [2048], P('dp')
- output 3: float32 [6291456], P('dp')
- output 4: float32 [1048576], P('dp')
- output 5: float32 [512], P('dp')
- output 6: float32 [131072], P('dp')
- output 7: float32 [1048576], P('dp')
- output 8: float32 [1048576], P('dp')
- output 9: float32 [4194304], P('dp')
All inputs are finite; a program needn't handle non-finite values.
Results may differ from the reference program's by a relative error of at most 0.0100842.
Values sent between devices are 32-bit elements.
A program may use at most 1 GiB of HBM per device.

```python
import jax
import jax.numpy as jnp
from jax import lax

DP = 32
B_DEV = 16
SEQ = 192
D = 2048
HEADS = 16
KV_RANK = 512
NOPE = 128
ROPE = 64
VHEAD = 128

QK = NOPE + ROPE
BATCH = DP * B_DEV
EPS = 1e-6
ROPE_BASE = 10000.0


def setup_inputs(seed: int = 0) -> dict:
    key_list = jax.random.split(jax.random.key(seed), 10)

    def draw_normal(key_no, shape, scale):
        return (jax.random.normal(key_list[key_no], shape, jnp.float32) * scale).astype(jnp.bfloat16)

    def draw_gain(key_no, width):
        return (1.0 + 0.3 * jax.random.normal(key_list[key_no], (width,), jnp.float32)).astype(jnp.bfloat16)

    return {
        'x_in': draw_normal(0, (BATCH, SEQ, D), 1.0),
        'grad_y': draw_normal(1, (BATCH, SEQ, D), 1.0),
        'g_in': draw_gain(2, D),
        'w_q': draw_normal(3, (D, HEADS, QK), D ** -0.5),
        'w_dkv': draw_normal(4, (D, KV_RANK), D ** -0.5),
        'g_kv': draw_gain(5, KV_RANK),
        'w_kr': draw_normal(6, (D, ROPE), D ** -0.5),
        'w_uk': draw_normal(7, (KV_RANK, HEADS, NOPE), KV_RANK ** -0.5),
        'w_uv': draw_normal(8, (KV_RANK, HEADS, VHEAD), KV_RANK ** -0.5),
        'w_o': draw_normal(9, (HEADS, VHEAD, D), (HEADS * VHEAD) ** -0.5),
    }


def rope_tables(seq_len, rot_dim):
    half_dim = rot_dim // 2
    inv_freq = jnp.power(ROPE_BASE, -2.0 * jnp.arange(half_dim, dtype=jnp.float32) / rot_dim)
    angles = jnp.arange(seq_len, dtype=jnp.float32)[:, None] * inv_freq[None, :]
    return jnp.cos(angles), jnp.sin(angles)


def apply_rope(vals, cos_t, sin_t):
    half_dim = vals.shape[-1] // 2
    first = vals[..., :half_dim]
    second = vals[..., half_dim:]
    return jnp.concatenate([first * cos_t - second * sin_t, second * cos_t + first * sin_t], axis=-1)


def rounded(vals):
    return vals.astype(jnp.bfloat16).astype(jnp.float32)


def block_forward(x_blk, params):
    g_in, w_q, w_dkv, g_kv, w_kr, w_uk, w_uv, w_o = params
    cos_t, sin_t = rope_tables(SEQ, ROPE)
    x_hat = x_blk * lax.rsqrt(jnp.mean(x_blk * x_blk, axis=-1, keepdims=True) + EPS)
    hidden = rounded(x_hat * g_in)
    q_full = jnp.einsum('bsd,dhk->bshk', hidden, w_q)
    q_nope = rounded(q_full[..., :NOPE])
    q_rot = rounded(apply_rope(q_full[..., NOPE:], cos_t[:, None, :], sin_t[:, None, :]))
    latent = jnp.einsum('bsd,dr->bsr', hidden, w_dkv)
    lat_hat = latent * lax.rsqrt(jnp.mean(latent * latent, axis=-1, keepdims=True) + EPS)
    lat_norm = rounded(lat_hat * g_kv)
    k_rot = rounded(apply_rope(jnp.einsum('bsd,de->bse', hidden, w_kr), cos_t, sin_t))
    k_nope = rounded(jnp.einsum('bsr,rhk->bshk', lat_norm, w_uk))
    v_heads = rounded(jnp.einsum('bsr,rhk->bshk', lat_norm, w_uv))
    scores = (jnp.einsum('bqhk,bthk->bhqt', q_nope, k_nope) + jnp.einsum('bqhe,bte->bhqt', q_rot, k_rot)) * (QK ** -0.5)
    positions = jnp.arange(SEQ)
    causal = positions[:, None] >= positions[None, :]
    attn_prob = rounded(jax.nn.softmax(jnp.where(causal, scores, -1e30), axis=-1))
    attn_out = rounded(jnp.einsum('bhqt,bthk->bqhk', attn_prob, v_heads))
    return x_blk + jnp.einsum('bshk,hkd->bsd', attn_out, w_o)


def reference(x_in, grad_y, g_in, w_q, w_dkv, g_kv, w_kr, w_uk, w_uv, w_o):
    params = tuple(weight.astype(jnp.float32) for weight in (g_in, w_q, w_dkv, g_kv, w_kr, w_uk, w_uv, w_o))
    x_dev = x_in.reshape(DP, B_DEV, SEQ, D)
    gy_dev = grad_y.reshape(DP, B_DEV, SEQ, D)

    def device_step(acc_grads, blocks):
        x_blk, gy_blk = blocks
        _, pullback = jax.vjp(block_forward, x_blk.astype(jnp.float32), params)
        dx_blk, d_params = pullback(gy_blk.astype(jnp.float32))
        acc_next = jax.tree.map(jnp.add, acc_grads, d_params)
        return acc_next, dx_blk.astype(jnp.bfloat16)

    zero_grads = jax.tree.map(jnp.zeros_like, params)
    grad_sums, dx_all = lax.scan(device_step, zero_grads, (x_dev, gy_dev))
    flat_grads = [(grad_sum / DP).reshape(-1) for grad_sum in grad_sums]
    return (dx_all.reshape(BATCH, SEQ, D), flat_grads[0], flat_grads[1], flat_grads[2], flat_grads[3],
            flat_grads[4], flat_grads[5], flat_grads[6], flat_grads[7])
```

```python
import functools

import jax
import jax.numpy as jnp
from jax import lax
from jax.experimental import pallas as pl
from jax.experimental.pallas import tpu as pltpu
from jax.sharding import PartitionSpec as P

EPS = 1e-6
ROPE_BASE = 10000.0
GROUPS = 2
BITS = ('c', 'x', 'y', 'z0', 'z1')


def contract(operand_a, operand_b, dim_a, dim_b):
    return lax.dot_general(operand_a, operand_b, (((dim_a,), (dim_b,)), ((), ())),
                           preferred_element_type=jnp.float32)


def rope_tables(seq_len, rot_dim):
    half_dim = rot_dim // 2
    inv_freq = jnp.power(ROPE_BASE, -2.0 * jnp.arange(half_dim, dtype=jnp.float32) / rot_dim)
    angles = jnp.arange(seq_len, dtype=jnp.float32)[:, None] * inv_freq[None, :]
    cos_t, sin_t = jnp.cos(angles), jnp.sin(angles)
    return jnp.concatenate([cos_t] * 4, axis=-1), jnp.concatenate([-sin_t, sin_t] * 2, axis=-1)


def swap_halves(vals, is_first):
    return jnp.where(is_first, pltpu.roll(vals, 96, 1), pltpu.roll(vals, 32, 1))


def split_cores(even, odd, low_half, first_core):
    low = jnp.where(low_half, even, pltpu.roll(odd, 64, 1)).astype(jnp.bfloat16)
    high = jnp.where(low_half, pltpu.roll(even, 64, 1), odd).astype(jnp.bfloat16)
    return jnp.where(first_core, high, low), jnp.where(first_core, low, high)


def norm_body(core_ref, x_ref, gain_ref, hidden_ref, send_ref, keep_ref):
    x_wide = x_ref[...].astype(jnp.float32)
    rows = x_wide.shape[0]
    inv_x = lax.rsqrt(jnp.mean(x_wide * x_wide, axis=-1, keepdims=True) + EPS)
    hidden = x_wide * inv_x * gain_ref[...]
    hidden_ref[...] = hidden.astype(jnp.bfloat16)
    low_half = lax.broadcasted_iota(jnp.int32, (rows, 128), 1) < 64
    for pair in range(hidden.shape[1] // 256):
        cols = slice(128 * pair, 128 * pair + 128)
        send_ref[:, cols], keep_ref[:, cols] = split_cores(
            hidden[:, 256 * pair:256 * pair + 128], hidden[:, 256 * pair + 128:256 * pair + 256], low_half, core_ref[0] == 0)


def normalize(core, x_in, gain, block=256):
    tokens, dim = x_in.shape

    def rows(width):
        return pl.BlockSpec((block, width), lambda i: (i, 0))

    return pl.pallas_call(
        norm_body,
        grid=(tokens // block,),
        in_specs=[pl.BlockSpec(memory_space=pltpu.SMEM), rows(dim), pl.BlockSpec((1, dim), lambda i: (0, 0))],
        out_specs=[rows(dim), rows(dim // 2), rows(dim // 2)],
        out_shape=[jax.ShapeDtypeStruct((tokens, width), jnp.bfloat16) for width in (dim, dim // 2, dim // 2)],
        compiler_params=pltpu.CompilerParams(dimension_semantics=('arbitrary',), vmem_limit_bytes=48 * 1024 * 1024),
        cost_estimate=pl.CostEstimate(flops=tokens * dim * 8, bytes_accessed=tokens * dim * 6, transcendentals=0),
    )(core, x_in, gain)


def attn_body(heads, qk_scale, core_ref, qn_ref, qr_ref, kr_ref, kn_ref, v_ref, do_ref, cos_ref, sin_ref,
              send_ref, keep_ref, dq_ref, dkv_ref, dkr_ref):
    seq_len = qn_ref.shape[0]
    lane = lax.broadcasted_iota(jnp.int32, (seq_len, 128), 1)
    is_first = (lane % 64) < 32
    low_half = lane < 64
    cos_t, sin_t = cos_ref[...], sin_ref[...]
    key_pos = lax.broadcasted_iota(jnp.int32, (seq_len, seq_len), 0)
    query_pos = lax.broadcasted_iota(jnp.int32, (seq_len, seq_len), 1)
    causal = key_pos <= query_pos
    kr_raw = kr_ref[...]
    k_rot = kr_raw * cos_t + swap_halves(kr_raw, is_first) * sin_t
    k_half = (jnp.where(low_half, k_rot, 0.0).astype(jnp.bfloat16), jnp.where(low_half, 0.0, k_rot).astype(jnp.bfloat16))
    dkr_sum = [None, None]
    for pair in range(heads // 2):
        rot_cols = slice(128 * pair, 128 * pair + 128)
        q_raw = qr_ref[:, rot_cols]
        q_rot = (q_raw * cos_t + swap_halves(q_raw, is_first) * sin_t).astype(jnp.bfloat16)
        dq_rot, outs = None, []
        for side in range(2):
            head = 2 * pair + side
            cols = slice(128 * head, 128 * head + 128)
            q_cat = jnp.concatenate([qn_ref[:, cols], q_rot], axis=1)
            k_cat = jnp.concatenate([kn_ref[:, cols], k_half[side]], axis=1)
            v_head = v_ref[:, cols]
            do_head = do_ref[:, cols]
            scores = jnp.where(causal, contract(k_cat, q_cat, 1, 1) * qk_scale, -1e30)
            expo = jnp.exp(scores - jnp.max(scores, axis=0, keepdims=True))
            prob = expo * (1.0 / jnp.sum(expo, axis=0, keepdims=True))
            prob_low = prob.astype(jnp.bfloat16)
            outs.append(contract(prob_low, v_head, 0, 0))
            d_prob = contract(v_head, do_head, 1, 1)
            row_dot = jnp.sum(prob * d_prob, axis=0, keepdims=True)
            d_scores = (prob * (d_prob - row_dot) * qk_scale).astype(jnp.bfloat16)
            d_v = contract(prob_low, do_head, 1, 0)
            d_k = contract(d_scores, q_cat, 1, 0)
            d_q = contract(d_scores, k_cat, 0, 0)
            dkv_ref[:, cols] = d_k[:, :128].astype(jnp.bfloat16)
            dkv_ref[:, slice(128 * (heads + head), 128 * (heads + head) + 128)] = d_v.astype(jnp.bfloat16)
            dq_ref[:, cols] = d_q[:, :128].astype(jnp.bfloat16)
            dq_rot = d_q[:, 128:] if dq_rot is None else dq_rot + d_q[:, 128:]
            dkr_sum[side] = d_k[:, 128:] if dkr_sum[side] is None else dkr_sum[side] + d_k[:, 128:]
        send_ref[:, rot_cols], keep_ref[:, rot_cols] = split_cores(outs[0], outs[1], low_half, core_ref[0] == 0)
        dq_back = dq_rot * cos_t - swap_halves(dq_rot, is_first) * sin_t
        dq_ref[:, slice(128 * heads + 128 * pair, 128 * heads + 128 * pair + 128)] = dq_back.astype(jnp.bfloat16)
    dk_rot = dkr_sum[0] + pltpu.roll(dkr_sum[1], 64, 1)
    dkr_ref[...] = dk_rot * cos_t - swap_halves(dk_rot, is_first) * sin_t


def attention(n_seq, seq_len, heads, qk_scale, core, q_nope, q_raw, k_raw, k_nope, v_heads, d_attn, cos_t, sin_t):
    tokens = n_seq * seq_len

    def rows(width):
        return pl.BlockSpec((seq_len, width), lambda i: (i, 0))

    table = pl.BlockSpec((seq_len, 128), lambda i: (0, 0))
    wide = heads * 128
    flops = n_seq * heads * seq_len * seq_len * 2 * (256 * 3 + 128 * 3)
    return pl.pallas_call(
        functools.partial(attn_body, heads, qk_scale),
        grid=(n_seq,),
        in_specs=[pl.BlockSpec(memory_space=pltpu.SMEM), rows(wide), rows(heads * 64), rows(128), rows(wide), rows(wide), rows(wide), table, table],
        out_specs=[rows(wide // 2), rows(wide // 2), rows(heads * 192), rows(2 * wide), rows(128)],
        out_shape=[jax.ShapeDtypeStruct((tokens, wide // 2), jnp.bfloat16),
                   jax.ShapeDtypeStruct((tokens, wide // 2), jnp.bfloat16),
                   jax.ShapeDtypeStruct((tokens, heads * 192), jnp.bfloat16),
                   jax.ShapeDtypeStruct((tokens, 2 * wide), jnp.bfloat16),
                   jax.ShapeDtypeStruct((tokens, 128), jnp.float32)],
        compiler_params=pltpu.CompilerParams(dimension_semantics=('arbitrary',), vmem_limit_bytes=48 * 1024 * 1024),
        cost_estimate=pl.CostEstimate(flops=flops, bytes_accessed=tokens * wide * 20, transcendentals=0),
    )(core, q_nope, q_raw, k_raw, k_nope, v_heads, d_attn, cos_t, sin_t)


def tail_body(n_in, n_weights, *refs):
    acts, weights = refs[:n_in], refs[n_in:n_in + n_weights]
    x_ref, gy_ref, gain_ref, gx_ref, dg_ref = refs[n_in + n_weights:n_in + n_weights + 3] + refs[-2:]
    blocks = [(act, start) for act, starts in zip(acts, ((0, 1024), (0, 1024), (0,))) for start in starts]
    d_hidden = None
    for (act, start), weight in zip(blocks, weights):
        term = contract(act[:, start:start + weight.shape[0]], weight[...], 1, 0)
        d_hidden = term if d_hidden is None else d_hidden + term
    x_wide = x_ref[...].astype(jnp.float32)
    inv_x = lax.rsqrt(jnp.mean(x_wide * x_wide, axis=-1, keepdims=True) + EPS)
    x_hat = x_wide * inv_x
    prod = d_hidden * x_hat
    gain = gain_ref[...]

    @pl.when(pl.program_id(0) == 0)
    def _():
        dg_ref[...] = jnp.zeros_like(dg_ref)

    dg_ref[...] += jnp.sum(prod, axis=0, keepdims=True)
    mean_dot = jnp.mean(prod * gain, axis=-1, keepdims=True)
    grad_x = gy_ref[...].astype(jnp.float32) + inv_x * (d_hidden * gain - x_hat * mean_dot)
    gx_ref[...] = grad_x.astype(jnp.bfloat16)


def tail(acts, weights, x_in, grad_y, gain, start, tokens, before, block=256):
    dim = x_in.shape[1]
    first = start // block

    def rows(width):
        return pl.BlockSpec((block, width), lambda i: (i + first, 0))

    def whole(arr):
        return pl.BlockSpec(arr.shape, lambda i: (0, 0), pipeline_mode=pl.Buffered(1))

    width = sum(act.shape[1] for act in acts)
    return pl.pallas_call(
        functools.partial(tail_body, len(acts), len(weights)),
        grid=(tokens // block,),
        in_specs=[rows(act.shape[1]) for act in acts] + [whole(weight) for weight in weights]
        + [rows(dim), rows(dim), pl.BlockSpec((1, dim), lambda i: (0, 0))] + [pl.BlockSpec(memory_space=pl.ANY)] * len(before),
        out_specs=[rows(dim), pl.BlockSpec((1, dim), lambda i: (0, 0))],
        input_output_aliases={len(acts) + len(weights) + 3: 0} if before else {},
        out_shape=[jax.ShapeDtypeStruct(x_in.shape, jnp.bfloat16), jax.ShapeDtypeStruct((1, dim), jnp.float32)],
        compiler_params=pltpu.CompilerParams(dimension_semantics=('arbitrary',), vmem_limit_bytes=58 * 1024 * 1024),
        cost_estimate=pl.CostEstimate(flops=2 * tokens * dim * width, bytes_accessed=tokens * (2 * width + 6 * dim) + 2 * width * dim,
                                      transcendentals=0),
    )(*acts, *weights, x_in, grad_y, gain, *before)


def solution(mesh):
    n_dev = mesh.shape['dp']
    perms = {name: [(dev, dev ^ (1 << pos)) for dev in range(n_dev)] for pos, name in enumerate(BITS)}

    def device_step(x_in, grad_y, g_in, w_q, w_dkv, g_kv, w_kr, w_uk, w_uv, w_o):
        me = lax.axis_index('dp')
        bit = {name: (me >> pos) & 1 for pos, name in enumerate(BITS)}

        def pick(arr, axis, index):
            return lax.dynamic_index_in_dim(arr, index, axis, keepdims=False)

        def exchange(addends, dims, name):
            axis = dims.index(name)
            send = sum(pick(arr, axis, 1 - bit[name]) for arr in addends)
            return send, [pick(arr, axis, bit[name]) for arr in addends], dims[:axis] + dims[axis + 1:]

        class Stream:
            def __init__(self, addends, dims, order):
                self.lanes, self.later = [(addends, dims, order)], ()
                self.fork()

            def sends(self):
                steps = [exchange(addends, dims, order[0]) for addends, dims, order in self.lanes]
                self.held = [(keep, dims, lane[2][0], lane[2][1:]) for (_, keep, dims), lane in zip(steps, self.lanes)]
                return [step[0] for step in steps]

            def transfer(self, values):
                return [lax.ppermute(value, 'dp', perms[held[2]]) for value, held in zip(values, self.held)]

            def receive(self, values):
                self.lanes = [(keep + [value], dims, order) for (keep, dims, _, order), value in zip(self.held, values)]
                self.fork()

            def fork(self):
                if len(self.lanes) == 1 and self.lanes[0][2] == () and 'x' in self.lanes[0][1]:
                    addends, dims, _ = self.lanes[0]
                    later = tuple(name for name in BITS[3:] if name in dims)
                    split = (addends[0].shape[-1] // 256) * 128
                    self.lanes = [([part[..., :split] for part in addends], dims, ('x', 'y') + later),
                                  ([part[..., split:] for part in addends], dims, ('y', 'x') + later)]

            def active(self):
                return bool(self.lanes[0][2])

            def result(self):
                return jnp.concatenate([sum(addends) for addends, _, _ in self.lanes], axis=-1)

        streams = []

        def launch(arr, names, order=()):
            rows = arr.shape[0] // (1 << len(names))
            streams.append(Stream([arr.reshape((2,) * len(names) + (rows, arr.shape[1]))], tuple(reversed(names)), order))
            return streams[-1]

        class Pair(Stream):
            def __init__(self, arr):
                self.value, self.open = arr, True
                streams.append(self)

            def sends(self):
                return [self.value]

            def transfer(self, values):
                return [lax.ppermute(values[0], 'dp', perms['c'])]

            def receive(self, values):
                self.value, self.open = values[0], False

            def active(self):
                return self.open

        def tick(work, *inputs):
            live = [stream for stream in streams if stream.active()]
            sends = [stream.sends() for stream in live]
            inputs, sends = lax.optimization_barrier((inputs, sends))
            arrived = [stream.transfer(values) for stream, values in zip(live, sends)]
            outs, arrived = lax.optimization_barrier((work(*inputs), arrived))
            for stream, values in zip(live, arrived):
                stream.receive(values)
            return outs

        def drain():
            while any(stream.active() for stream in streams):
                for stream in streams:
                    if stream.active():
                        stream.receive(stream.transfer(stream.sends()))

        n_seq, seq_len, dim = x_in.shape
        tokens = n_seq * seq_len
        heads, nope = w_uk.shape[1], w_uk.shape[2]
        rank = w_dkv.shape[1]
        rot = w_kr.shape[1]
        qk_scale = w_q.shape[2] ** -0.5
        group = heads // GROUPS
        cos_t, sin_t = rope_tables(seq_len, rot)
        x2 = x_in.reshape(tokens, dim)
        gy2 = grad_y.reshape(tokens, dim)
        gain_in = g_in.astype(jnp.float32)
        gain_kv = g_kv.astype(jnp.float32)
        core = bit['c'].astype(jnp.int32).reshape(1)
        hidden, h_send, h_keep = normalize(core, x2, gain_in[None, :])
        w_side = jnp.concatenate([w_dkv, w_kr, w_kr], axis=1)
        side = contract(hidden, w_side, 1, 0)
        latent, k_raw = side[:, :rank], side[:, rank:]
        inv_lat = lax.rsqrt(jnp.mean(latent * latent, axis=-1, keepdims=True) + EPS)
        lat_hat = latent * inv_lat
        lat_norm = (lat_hat * gain_kv).astype(jnp.bfloat16)
        w_o2 = w_o.reshape(heads * nope, dim)

        lat_norm = lax.optimization_barrier(lat_norm)
        w_groups, w_parts = [], []
        for g in range(GROUPS):
            hs = slice(g * group, (g + 1) * group)
            w_nope = w_q[:, hs, :nope].reshape(dim, group * nope)
            w_rot = w_q[:, hs, nope:].reshape(dim, group * rot)
            w_groups.extend([w_nope.T, w_rot.T])
            w_parts.append((w_nope, w_rot, w_uk[:, hs].reshape(rank, group * nope), w_uv[:, hs].reshape(rank, group * nope),
                            w_o2[g * group * nope:(g + 1) * group * nope]))

        def project_q(g, hidden):
            return (contract(hidden, w_parts[g][0], 1, 0).astype(jnp.bfloat16), contract(hidden, w_parts[g][1], 1, 0))

        def project_kv(g, lat_norm, gy2):
            return (contract(lat_norm, w_parts[g][2], 1, 0).astype(jnp.bfloat16),
                    contract(lat_norm, w_parts[g][3], 1, 0).astype(jnp.bfloat16),
                    contract(gy2, w_parts[g][4], 1, 1).astype(jnp.bfloat16))

        def attend(q_nope, q_raw, k_raw, k_nope, v_heads, d_attn):
            return attention(n_seq, seq_len, group, qk_scale, core, q_nope, q_raw, k_raw, k_nope, v_heads, d_attn, cos_t, sin_t)

        def outer(*pairs):
            return [contract(pairs[i], pairs[i + 1], 0, 0) for i in range(0, len(pairs), 2)]

        def outer_add(left, right, received):
            return contract(left, right, 0, 0) + received

        def latent_back(d_kv0, d_kv1, dkr0, dkr1, lat_hat, inv_lat):
            d_lat = sum(contract(d_kv, jnp.concatenate(w_parts[g][2:4], axis=1), 1, 1) for g, d_kv in enumerate((d_kv0, d_kv1)))
            d_g_kv = jnp.sum(d_lat * lat_hat, axis=0)
            d_lat_hat = d_lat * gain_kv
            d_latent = inv_lat * (d_lat_hat - lat_hat * jnp.mean(d_lat_hat * lat_hat, axis=-1, keepdims=True))
            lane_ok = jnp.arange(2 * rot) < rot
            d_side = jnp.concatenate([d_latent, jnp.where(lane_ok, dkr0 + dkr1, 0.0)], axis=1).astype(jnp.bfloat16)
            return d_g_kv, d_side

        q_parts = project_q(0, hidden)
        kv_parts = project_kv(0, lat_norm, gy2)
        CHIP = BITS[1:]
        o_send, o_keep, d_q0, d_kv0, dkr0 = attend(*q_parts, k_raw, *kv_parts)
        pair_q = Pair(lax.optimization_barrier(outer(h_send, d_q0))[0])
        wo_send, d_wkv = tick(outer, o_send, gy2, lat_norm, d_kv0)
        pair_o, shards_kv = Pair(wo_send), [launch(d_wkv, BITS, ('c',))]
        shards_q = [launch(tick(outer_add, h_keep, d_q0, pair_q.value), CHIP)]
        d_wo, q_parts = tick(lambda left, right, received, hidden: (outer_add(left, right, received), project_q(1, hidden)),
                             o_keep, gy2, pair_o.value, hidden)
        shards_o = [launch(d_wo, CHIP[:3])]
        kv_parts = tick(functools.partial(project_kv, 1), lat_norm, gy2)
        o_send, o_keep, d_q1, d_kv1, dkr1 = tick(attend, *q_parts, k_raw, *kv_parts)
        pair_q = Pair(tick(outer, h_send, d_q1)[0])
        wo_send, d_wkv = tick(outer, o_send, gy2, lat_norm, d_kv1)
        pair_o = Pair(wo_send)
        shards_kv.append(launch(d_wkv, BITS, ('c',)))
        shards_q.append(launch(tick(outer_add, h_keep, d_q1, pair_q.value), CHIP))
        d_wo, (d_g_kv, d_side) = tick(lambda left, right, received, *rest: (outer_add(left, right, received), latent_back(*rest)),
                                      o_keep, gy2, pair_o.value, d_kv0, d_kv1, dkr0, dkr1, lat_hat, inv_lat)
        shards_o.append(launch(d_wo, CHIP[:3]))
        third = tokens // 3

        def tail_part(part, before, *acts):
            return tail(acts, w_groups + [w_side.T], x2, gy2, gain_in[None, :], part * third, third, before)

        d_wside, (grad_x, d_g_in) = tick(lambda hidden, *acts: (contract(hidden, acts[-1], 0, 0), tail_part(0, (), *acts)),
                                         hidden, d_q0, d_q1, d_side)
        shard_side = launch(d_wside, BITS, ('c',))
        for part in range(1, 3):
            grad_x, d_g_part = tick(lambda before, *acts: tail_part(part, (before,), *acts), grad_x, d_q0, d_q1, d_side)
            d_g_in = d_g_in + d_g_part
        small = jnp.concatenate([d_g_in.reshape(n_dev, -1), d_g_kv.reshape(n_dev, -1)], axis=1)
        small = jnp.pad(small, ((0, 0), (0, 128 - small.shape[1]))).reshape((2,) * 5 + (1, 128))
        addends, dims = [small], tuple(reversed(BITS))
        for name in BITS:
            send, keep, dims = exchange(addends, dims, name)
            addends = keep + [lax.ppermute(send, 'dp', perms[name])]
        small = sum(addends)[0] / n_dev
        drain()
        low, high = [shard.result() for shard in shards_o]
        mine = jnp.where(bit['z1'] == 0, low, high)
        d_w_o = mine + lax.ppermute(jnp.where(bit['z1'] == 0, high, low), 'dp', perms['z1'])
        shards_q = [shard.result() for shard in shards_q]
        shards_kv = [shard.result() for shard in shards_kv]
        shard_side = shard_side.result()

        per_in, per_kv = dim // n_dev, rank // n_dev
        inv_dev = 1.0 / n_dev
        q_parts = [jnp.concatenate([shard[:, :group * nope].reshape(-1, group, nope),
                                    shard[:, group * nope:].reshape(-1, group, rot)], axis=-1) for shard in shards_q]
        d_w_q = jnp.concatenate(q_parts, axis=1).reshape(-1) * inv_dev
        d_w_uk = jnp.concatenate([shard[:, :group * nope] for shard in shards_kv], axis=1).reshape(-1) * inv_dev
        d_w_uv = jnp.concatenate([shard[:, group * nope:] for shard in shards_kv], axis=1).reshape(-1) * inv_dev
        return (grad_x.reshape(x_in.shape), small[:per_in], d_w_q, shard_side[:, :rank].reshape(-1) * inv_dev,
                small[per_in:per_in + per_kv], shard_side[:, rank:rank + rot].reshape(-1) * inv_dev,
                d_w_uk, d_w_uv, d_w_o.reshape(-1) * inv_dev)

    batch_spec = P('dp')
    full_spec = P()
    return jax.shard_map(device_step, mesh=mesh,
                         in_specs=(batch_spec, batch_spec) + (full_spec,) * 8,
                         out_specs=(batch_spec,) * 9, check_vma=False)
```
